32 devices in a mesh: mesh: 4 (over y, x), sub: 8 (over z, core).
Axes of the slice: x: 2, y: 2, z: 4, core: 2. Of those that a mesh axis runs over, the one named last changes fastest.
Arguments:
- displacement: float32 [3, 2, 32, 1024], P(None, None, 'mesh', 'sub'), may hold values from -4 to 4
- velocity: float32 [3, 2, 32, 1024], P(None, None, 'mesh', 'sub'), may hold values from -6 to 6
- node_mass: float32 [2, 32, 1024], P(None, 'mesh', 'sub'), may hold values from 0.5 to 2
- moduli: float32 [2, 32, 1024], P(None, 'mesh', 'sub'), may hold values from 0.5 to 2
- stiffness: float32 [24, 24], replicated, may hold values from -0.45 to 12, as said below
- surface_ref: float32 [3, 32, 1024], P(None, 'mesh', 'sub'), may hold values from -6 to 6
- facets: float32 [4, 8, 6, 1024], P('mesh', 'sub'), may hold values from -6 to 6
- penalty: float32 [4, 8, 1024], P('mesh', 'sub'), may hold values from 0.5 to 4
- owners: int32 [2, 4, 8, 8, 1], P(None, 'mesh', 'sub'), may hold values from 0 to 3; in each aligned block of 8 rows (0 to 7, 8 to 15, ..., all dimensions but the last counted through in order) at most 4 rows name the same one
- facet_pairs: int32 [2, 32, 1024], P(None, 'mesh', 'sub'), may hold values from 0 to 1023
Outputs:
- final_displacement: float32 [3, 2, 32, 1024], P(None, None, 'mesh', 'sub')
- final_velocity: float32 [3, 2, 32, 1024], P(None, None, 'mesh', 'sub')
The draws below stay inside these ranges and needn't reach their ends.
Inputs may be any that keep to these rules, and one draw needn't show every extreme that they name: `owners`: in every step no device sends more than 4 of its blocks to one owner, and some device sends exactly 4 to one owner. `stiffness`: Symmetric.
All inputs are finite; a program needn't handle non-finite values.
Results may differ from the reference program's by a relative error of at most 0.0001.
Values sent between devices are 32-bit elements; how exact they have to be, the bound alone decides.
A program may use at most 64 MiB of HBM per device.

```python
import math
import jax
import jax.numpy as jnp
import numpy as np
from jax import lax

NZ = 2
BLOCK = 128
TF = 1024
STEPS = 2
OWNERS = 4
SUBPARTS = 8
SB = 8
CAP = 4
NX = 32
NY = 1024
N_MESH = 4


def draw_stiffness(key, part):
    key_off = jax.random.fold_in(key, 11)
    key_diag = jax.random.fold_in(key, 12)
    sampled = jax.random.truncated_normal(key_off, -3.0, 3.0, (24, 24), jnp.float32) * 0.15
    symmetric = (sampled + sampled.T) * 0.5
    off_diagonal = symmetric * (1.0 - jnp.eye(24, dtype=jnp.float32))
    surplus = jax.random.uniform(key_diag, (24,), jnp.float32, 0.5, 1.5)
    return off_diagonal + jnp.diag(jnp.sum(jnp.abs(off_diagonal), axis=1) + surplus)


def touch_ends(entries, own_key, least, high):
    shape = entries.shape
    index_at = [jax.random.randint(jax.random.fold_in(own_key, axis), (), 0, shape[axis]) for axis in range(len(shape))]
    entries = entries.at[tuple(index_at)].set(least)
    longest = shape.index(max(shape))
    index_at[longest] = (index_at[longest] + 1) % shape[longest]
    return entries.at[tuple(index_at)].set(high)


def steps_of(rng, dims, cuts, least, high):
    def one(position, shards_of):
        draws = jax.random.uniform(jax.random.fold_in(jax.random.fold_in(rng, 6), position), (shards_of,), jnp.float32, least / len(cuts), high / len(cuts))
        return jnp.repeat(jnp.exp(draws), dims[position] // shards_of).reshape((-1,) + (1,) * (len(dims) - position - 1))

    gain = one(*cuts[0])
    for cut in cuts[1:]:
        gain = gain * one(*cut)
    return gain


def assign_block(stream_key, own, number, rows, number_of, top, reach, slope):
    order = jax.random.permutation(stream_key, number_of)
    heavy_load, usual = shares(number_of, rows * top, reach, slope, True), shares(number_of, rows * top, reach, slope, False)
    places = jnp.arange(number_of)

    def named(tallies, offset_by):
        used = int((tallies > 0).sum())
        fixed = max(1, used // 4)
        moved = fixed + (places - fixed + offset_by * (used - fixed)) % max(1, number_of - fixed)
        return jnp.zeros((number_of,), jnp.int32).at[order[jnp.where(places < fixed, places, moved)]].set(jnp.asarray(tallies, jnp.int32))

    tallies = jnp.where(number % 4 == 0, named(heavy_load, number // 4), named(usual, number - number // 4 - 1))
    mixed = jax.random.permutation(jax.random.fold_in(own, 3), number_of)
    source_of, taker = mixed[0:number_of // 2 * 2:2], mixed[1:number_of // 2 * 2:2]
    margin = jnp.minimum(tallies[source_of] - 1, reach - tallies[taker]) // 2
    margin = jnp.where((source_of == order[0]) | (taker == order[0]) | (tallies[taker] == 0), 0, jnp.maximum(margin, 0))
    moved = jax.random.randint(jax.random.fold_in(own, 4), (number_of // 2,), 0, 1 << 20) % (margin + 1)
    tallies = tallies.at[source_of].add(-moved).at[taker].add(moved)
    labels = jnp.searchsorted(jnp.cumsum(tallies), jnp.arange(rows * top), side="right").astype(jnp.int32)
    listing = labels.reshape(top, rows).T
    listing = listing[jax.random.permutation(jax.random.fold_in(own, 1), rows)]
    offset_by = jax.random.randint(jax.random.fold_in(own, 2), (rows, 1), 0, top)
    return jnp.take_along_axis(listing, (jnp.arange(top)[None, :] + offset_by) % top, axis=1)


def shares(amount, total, reach, lean, full):
    portions = [(1 << 20) // math.isqrt(rank ** lean) + 1 for rank in range(1, amount + 1)]
    largest = reach if full else min(reach, max(-(-total // amount), total * portions[0] // sum(portions)))
    least = 1 if total - largest >= amount - 1 else 0
    given, spare = [largest] + [least] * (amount - 1), total - largest - least * (amount - 1)
    while spare > 0:
        free = [i for i in range(1, amount) if given[i] < largest] or [i for i in range(1, amount) if given[i] < reach]
        whole, remaining = sum([portions[i] for i in free]), spare
        for i in free:
            more = min(reach - given[i], max(1, remaining * portions[i] // whole), spare)
            given[i] = given[i] + more
            spare = spare - more
    return np.array(given)


def bell_draw(rng, shape, width, bound, cuts=(), held_as=jnp.bfloat16):
    array = width * jax.random.normal(rng, shape, jnp.float32)
    if cuts:
        array = array * steps_of(rng, shape, cuts, -0.22, 0.18)
    return jnp.clip(array, -bound, bound).astype(held_as)


def setup_inputs(seed: int = 0) -> dict:
    arg_keys = jax.random.split(jax.random.key(seed), 11)
    displacement = bell_draw(arg_keys[0], (3, NZ, NX, NY), 0.3, 4.0, ((2, 4), (3, 8)), jnp.float32)
    velocity = bell_draw(arg_keys[1], (3, NZ, NX, NY), 1.0, 6.0, ((2, 4), (3, 8)), jnp.float32)
    node_mass = jnp.clip(jnp.exp(math.log(2.0) - 1.3862944 * jax.random.uniform(arg_keys[2], (NZ, NX, NY), jnp.float32) ** steps_of(arg_keys[2], (NZ, NX, NY), ((1, 4), (2, 8)), -0.2, 0.2)), 0.5, 2.0)
    moduli = jnp.clip(jnp.exp(math.log(2.0) - 1.3862944 * jax.random.uniform(arg_keys[3], (NZ, NX, NY), jnp.float32) ** steps_of(arg_keys[3], (NZ, NX, NY), ((1, 4), (2, 8)), -0.2, 0.2)), 0.5, 2.0)
    stiffness = draw_stiffness(jax.random.fold_in(arg_keys[10], 71), 0)
    surface_ref = bell_draw(arg_keys[5], (3, NX, NY), 1.0, 6.0, ((1, 4), (2, 8)), jnp.float32)
    facets = bell_draw(arg_keys[6], (OWNERS, SUBPARTS, 6, TF), 1.0, 6.0, ((0, 4), (1, 8)), jnp.float32)
    penalty = jnp.clip(jnp.exp(math.log(4.0) - 2.0794415 * jax.random.uniform(arg_keys[7], (OWNERS, SUBPARTS, TF), jnp.float32) ** steps_of(arg_keys[7], (OWNERS, SUBPARTS, TF), ((0, 4), (1, 8)), -0.2, 0.2)), 0.5, 4.0)
    owners_keys = jax.random.split(jax.random.fold_in(arg_keys[8], 1), STEPS * OWNERS * SUBPARTS * SB // SB)
    owners_turns = jax.random.permutation(jax.random.fold_in(arg_keys[8], 3), STEPS * OWNERS * SUBPARTS * SB // SB)
    owners = jax.vmap(lambda own, number: assign_block(jax.random.fold_in(arg_keys[8], 2), own, number, SB, OWNERS, 1, CAP, 2))(owners_keys, owners_turns).reshape((STEPS, OWNERS, SUBPARTS, SB, 1))
    facet_pairs = touch_ends(jax.random.randint(arg_keys[9], (STEPS, NX, NY), 0, TF), jax.random.fold_in(arg_keys[9], 1), 0, TF - 1).astype(jnp.int32)
    return dict(displacement=displacement, velocity=velocity, node_mass=node_mass, moduli=moduli, stiffness=stiffness, surface_ref=surface_ref, facets=facets, penalty=penalty, owners=owners, facet_pairs=facet_pairs)


TIME_STEP = 0.1
CORNER_SHIFTS = ((0, 0, 0), (0, 0, 1), (0, 1, 0), (0, 1, 1), (1, 0, 0), (1, 0, 1), (1, 1, 0), (1, 1, 1))


def node_forces(node_patch, patch_moduli, stiffness):
    layers = node_patch.shape[1]
    row_count = node_patch.shape[2] - 2
    col_count = node_patch.shape[3] - 2
    element_scale = jnp.zeros((layers - 1, row_count + 1, col_count + 1), jnp.float32)
    corners = []
    for shift_z, shift_x, shift_y in CORNER_SHIFTS:
        element_scale = element_scale + patch_moduli[shift_z:shift_z + layers - 1, shift_x:shift_x + row_count + 1, shift_y:shift_y + col_count + 1]
        corners.append(node_patch[:, shift_z:shift_z + layers - 1, shift_x:shift_x + row_count + 1, shift_y:shift_y + col_count + 1])
    element_scale = element_scale * 0.125
    stacked = jnp.concatenate(corners, axis=0).reshape(24, -1)
    forces = jnp.dot(stiffness, stacked, precision=lax.Precision.HIGHEST).reshape(24, layers - 1, row_count + 1, col_count + 1) * element_scale[None]
    summed = jnp.zeros((3, layers, row_count, col_count), jnp.float32)
    for corner, (shift_z, shift_x, shift_y) in enumerate(CORNER_SHIFTS):
        contribution = forces[3 * corner:3 * corner + 3, :, 1 - shift_x:1 - shift_x + row_count, 1 - shift_y:1 - shift_y + col_count]
        summed = summed.at[:, shift_z:shift_z + layers - 1].add(contribution)
    return summed


def contact_push(points, facet_rows, stiffness_row):
    normal_gap = jnp.sum(facet_rows[3:6] * (points - facet_rows[0:3]), axis=0)
    return facet_rows[3:6] * (stiffness_row * jnp.maximum(-normal_gap, 0.0))[None]


def internal_forces(displacement, moduli, stiffness):
    padded = jnp.pad(displacement, ((0, 0), (0, 0), (1, 1), (1, 1)), mode="wrap")
    padded_moduli = jnp.pad(moduli, ((0, 0), (1, 1), (1, 1)), mode="wrap")
    row_count = displacement.shape[2] // N_MESH

    def one_block(block_index):
        row_start = block_index * row_count
        node_patch = lax.dynamic_slice_in_dim(padded, row_start, row_count + 2, 2)
        patch_moduli = lax.dynamic_slice_in_dim(padded_moduli, row_start, row_count + 2, 1)
        return node_forces(node_patch, patch_moduli, stiffness)

    pieces = lax.map(one_block, jnp.arange(N_MESH, dtype=jnp.int32))
    return pieces.transpose(1, 2, 0, 3, 4).reshape(displacement.shape)


def contact_forces(positions, owner_step, pair_step, facets, penalty):
    groups = facets.shape[0]
    sub_count = facets.shape[1]
    table_width = facets.shape[3]
    row_count = positions.shape[1] // groups
    col_count = positions.shape[2] // sub_count
    points = positions.reshape(3, groups, row_count, sub_count, col_count).transpose(0, 1, 3, 2, 4).reshape(3, -1)
    pair_rows = pair_step.reshape(groups, row_count, sub_count, col_count).transpose(0, 2, 1, 3).reshape(groups, sub_count, -1)
    per_point = jnp.repeat(owner_step[..., 0], BLOCK, axis=2)
    sub_index = jnp.arange(sub_count, dtype=jnp.int32)[None, :, None]
    flat_index = ((per_point * sub_count + sub_index) * table_width + pair_rows).reshape(-1).astype(jnp.int32)
    whole_table = facets.transpose(2, 0, 1, 3).reshape(6, -1)
    facet_rows = jnp.take(whole_table, flat_index, axis=1)
    pushed = contact_push(points, facet_rows, jnp.take(penalty.reshape(-1), flat_index))
    return pushed.reshape(3, groups, sub_count, row_count, col_count).transpose(0, 1, 3, 2, 4).reshape(positions.shape)


def reference(displacement, velocity, node_mass, moduli, stiffness, surface_ref, facets, penalty, owners, facet_pairs):
    for step_index in range(STEPS):
        internal = internal_forces(displacement, moduli, stiffness)
        pushed = contact_forces(surface_ref + displacement[:, 0], owners[step_index], facet_pairs[step_index], facets, penalty)
        net_force = (-internal).at[:, 0].add(pushed)
        velocity = velocity + TIME_STEP * net_force / node_mass[None]
        displacement = displacement + TIME_STEP * velocity
    return displacement, velocity
```

```python
import functools

import jax
import jax.numpy as jnp
from jax import lax
from jax.experimental import pallas as pl
from jax.experimental.pallas import tpu as pltpu
from jax.sharding import PartitionSpec as P

TIME_STEP = 0.1
MESH = pl.DeviceIdType.MESH
ROWS = 8
LANES = 128
DIRECTIONS = ((0, 1), (0, -1), (1, 0), (-1, 0), (1, 1), (1, -1), (-1, 1), (-1, -1))
SLOT = {d: i for i, d in enumerate(DIRECTIONS)}
PAD = 24


def kernel(
    n_mesh,
    n_sub,
    steps,
    stiff,
    owners,
    disp_hbm,
    vel_hbm,
    mass_hbm,
    moduli_hbm,
    surf_hbm,
    facets_hbm,
    penalty_hbm,
    pairs_hbm,
    out_disp,
    out_vel,
    own,
    vel,
    mass,
    surf,
    pairs,
    table,
    pen,
    packed,
    arrived,
    wide,
    found,
    local_sem,
    table_send,
    table_recv,
    pen_send,
    pen_recv,
    halo_send,
    halo_recv,
):
    q, s = lax.axis_index("mesh"), lax.axis_index("sub")

    def at(dq, ds):
        return (lax.rem(q + dq + n_mesh, n_mesh), lax.rem(s + ds + n_sub, n_sub))

    copies = [
        pltpu.make_async_copy(src, dst, local_sem.at[i])
        for i, (src, dst) in enumerate(
            (
                (disp_hbm, own.at[pl.ds(0, 48)]),
                (moduli_hbm, own.at[pl.ds(48, 16)]),
                (facets_hbm, table.at[q]),
                (penalty_hbm, pen.at[q]),
                (pairs_hbm, pairs),
                (surf_hbm, surf),
                (vel_hbm, vel),
                (mass_hbm, mass),
            )
        )
    ]
    barrier = pltpu.get_barrier_semaphore()
    partners = [at(*d) for d in DIRECTIONS if d[1] != 0] + [at(d, 0) for d in range(1, n_mesh)]
    for device in partners:
        pl.semaphore_signal(barrier, inc=1, device_id=device, device_id_type=MESH)
    for copy in copies:
        copy.start()

    lane = lax.broadcasted_iota(jnp.int32, (ROWS, LANES), 1)

    def pack(step, planes, count):
        left = jnp.zeros((ROWS, LANES), jnp.float32)
        right = left
        for p in range(count):
            plane = planes[p]
            left = jnp.where(lane == p, pltpu.roll(plane, p, 1) if p else plane, left)
            right = jnp.where(lane == p, pltpu.roll(plane, p + 1, 1), right)
        packed[step, 0] = left
        packed[step, 1] = right
        packed[step, 2] = own[pl.ds(0, 8, stride=8), :]
        packed[step, 3] = own[pl.ds(7, 8, stride=8), :]

    def halo(step):
        made = []
        for i, (dq, ds) in enumerate(DIRECTIONS):
            source = (2 if dq < 0 else 3) if dq else (0 if ds < 0 else 1)
            made.append(
                pltpu.make_async_remote_copy(
                    src_ref=packed.at[step, source],
                    dst_ref=arrived.at[step, i],
                    send_sem=halo_send.at[step, i],
                    recv_sem=halo_recv.at[step, i],
                    device_id=at(dq, ds),
                    device_id_type=MESH,
                )
            )
        return made

    copies[0].wait()
    copies[1].wait()
    pack(0, [own[pl.ds(8 * p, 8), :] for p in range(8)], 8)
    copies[2].wait()
    copies[3].wait()
    pl.semaphore_wait(barrier, len(partners))
    halos = halo(0)
    for copy in halos:
        copy.start()
    shared = []
    for d in range(1, n_mesh):
        for ref, send, recv in ((table, table_send, table_recv), (pen, pen_send, pen_recv)):
            shared.append(
                pltpu.make_async_remote_copy(
                    src_ref=ref.at[q],
                    dst_ref=ref.at[q],
                    send_sem=send.at[d - 1],
                    recv_sem=recv.at[d - 1],
                    device_id=at(d, 0),
                    device_id_type=MESH,
                )
            )
    for copy in shared:
        copy.start()
    for copy in copies[4:]:
        copy.wait()
    inverse = [TIME_STEP / mass[pl.ds(8 * a, 8), :] for a in range(2)]

    def gather(step):
        for b in range(ROWS):
            owner = owners[step, b]
            index = jnp.broadcast_to(pairs[pl.ds(step * ROWS + b, 1), :], (ROWS, LANES))
            chunk, place = index >> 7, index & 127
            total = jnp.zeros((ROWS, LANES), jnp.float32)
            for k in range(table.shape[2] // LANES):
                columns = pl.ds(k * LANES, LANES)
                stiffness_row = pen[owner, :, columns]
                rows = jnp.concatenate([table[owner, :, columns], stiffness_row, stiffness_row], axis=0)
                picked = jnp.take_along_axis(rows, place, axis=1, mode="promise_in_bounds")
                total = jnp.where(chunk == k, picked, total)
            found[step, pl.ds(8 * b, 8), :] = total

    def spread(step, planes, count):
        from_left, from_right = arrived[step, SLOT[(0, 1)]], arrived[step, SLOT[(0, -1)]]
        for p in range(count):
            plane = planes[p]
            before = pltpu.roll(from_left, LANES - p, 1) if p else from_left
            after = pltpu.roll(from_right, LANES - 1 - p, 1)
            rows = pl.ds(p * PAD + 8, 8)
            wide[0, rows, :] = jnp.where(lane == 0, before, pltpu.roll(plane, 1, 1))
            wide[1, rows, :] = plane
            wide[2, rows, :] = jnp.where(lane == LANES - 1, after, pltpu.roll(plane, LANES - 1, 1))
        for dq, row in ((1, 7), (-1, 16)):
            centre = arrived[step, SLOT[(dq, 0)]]
            west, east = arrived[step, SLOT[(dq, 1)]], arrived[step, SLOT[(dq, -1)]]
            rows = pl.ds(row, 8, stride=PAD)
            wide[0, rows, :] = pltpu.roll(jnp.where(lane == LANES - 1, west, centre), 1, 1)
            wide[1, rows, :] = centre
            wide[2, rows, :] = pltpu.roll(jnp.where(lane == 0, east, centre), LANES - 1, 1)

    def shifted(p, di, dj):
        return wide[dj + 1, pl.ds(p * PAD + 8 + di, 8), :]

    scales = {}
    planes = [own[pl.ds(8 * p, 8), :] for p in range(8)]
    for step in range(steps):
        if step == 0:
            for copy in shared:
                copy.wait_recv()
        gather(step)
        for copy in halos:
            copy.wait_recv()
        spread(step, planes, 8 if step == 0 else 6)
        if step == 0:
            both = {
                (di, dj): shifted(6, di, dj) + shifted(7, di, dj) for di in (-1, 0, 1) for dj in (-1, 0, 1)
            }
            for b in (0, 1):
                for e in (0, 1):
                    scales[b, e] = 0.125 * (
                        (both[-b, -e] + both[-b, 1 - e]) + (both[1 - b, -e] + both[1 - b, 1 - e])
                    )
        force = [None] * 6
        for b in (0, 1):
            for e in (0, 1):
                sums = [None] * 6
                for corner in range(8):
                    a2, b2, e2 = corner >> 2, (corner >> 1) & 1, corner & 1
                    for m2 in range(3):
                        value = shifted(2 * m2 + a2, b2 - b, e2 - e)
                        for a in (0, 1):
                            for m in range(3):
                                row = 3 * (4 * a + 2 * b + e) + m
                                term = stiff[row, 3 * corner + m2] * value
                                o = 2 * m + a
                                sums[o] = term if sums[o] is None else sums[o] + term
                for o in range(6):
                    term = scales[b, e] * sums[o]
                    force[o] = term if force[o] is None else force[o] + term
        facet = [found[step, pl.ds(c, 8, stride=8), :] for c in range(7)]
        points = [surf[pl.ds(8 * m, 8), :] + planes[2 * m] for m in range(3)]
        gap = sum(facet[3 + m] * (points[m] - facet[m]) for m in range(3))
        strength = facet[6] * jnp.maximum(-gap, 0.0)
        last = step == steps - 1
        fresh = []
        for o in range(6):
            m, a = o // 2, o % 2
            net = facet[3 + m] * strength - force[o] if a == 0 else -force[o]
            rows = pl.ds(8 * o, 8)
            speed = vel[rows, :] + inverse[a] * net
            moved = planes[o] + TIME_STEP * speed
            fresh.append(moved)
            if last:
                out_vel[rows, :] = speed
                out_disp[rows, :] = moved
            else:
                vel[rows, :] = speed
                own[rows, :] = moved
        for copy in halos:
            copy.wait_send()
        planes = fresh
        if not last:
            pack(step + 1, planes, 6)
            halos = halo(step + 1)
            for copy in halos:
                copy.start()
    for copy in shared:
        copy.wait_send()


def shards(
    displacement,
    velocity,
    node_mass,
    moduli,
    stiffness,
    surface_ref,
    facets,
    penalty,
    owners,
    facet_pairs,
):
    steps = owners.shape[0]
    width = facets.shape[3]
    n_mesh, n_sub = lax.axis_size("mesh"), lax.axis_size("sub")
    assert displacement.shape == (3, 2, ROWS, LANES)
    f32 = jnp.float32
    out = jax.ShapeDtypeStruct((6 * ROWS, LANES), f32)
    smem = pl.BlockSpec(memory_space=pltpu.SMEM)
    anywhere = pl.BlockSpec(memory_space=pl.ANY)
    vmem = pl.BlockSpec(memory_space=pltpu.VMEM)
    dma = pltpu.SemaphoreType.DMA
    moved, speed = pl.pallas_call(
        functools.partial(kernel, n_mesh, n_sub, steps),
        out_shape=(out, out),
        in_specs=[smem, smem] + [anywhere] * 8,
        out_specs=(vmem, vmem),
        scratch_shapes=[
            pltpu.VMEM((8 * ROWS, LANES), f32),
            pltpu.VMEM((6 * ROWS, LANES), f32),
            pltpu.VMEM((2 * ROWS, LANES), f32),
            pltpu.VMEM((3 * ROWS, LANES), f32),
            pltpu.VMEM((steps * ROWS, LANES), jnp.int32),
            pltpu.VMEM((n_mesh, 6, width), f32),
            pltpu.VMEM((n_mesh, 1, width), f32),
            pltpu.VMEM((steps, 4, ROWS, LANES), f32),
            pltpu.VMEM((steps, 8, ROWS, LANES), f32),
            pltpu.VMEM((3, 8 * PAD, LANES), f32),
            pltpu.VMEM((steps, 8 * ROWS, LANES), f32),
            dma((8,)),
            dma((n_mesh - 1,)),
            dma((n_mesh - 1,)),
            dma((n_mesh - 1,)),
            dma((n_mesh - 1,)),
            dma((steps, 8)),
            dma((steps, 8)),
        ],
        compiler_params=pltpu.CompilerParams(collective_id=0, has_side_effects=True),
    )(
        stiffness,
        owners.reshape(steps, ROWS),
        displacement.reshape(6 * ROWS, LANES),
        velocity.reshape(6 * ROWS, LANES),
        node_mass.reshape(2 * ROWS, LANES),
        moduli.reshape(2 * ROWS, LANES),
        surface_ref.reshape(3 * ROWS, LANES),
        facets.reshape(6, width),
        penalty.reshape(1, width),
        facet_pairs.reshape(steps * ROWS, LANES),
    )
    return moved.reshape(displacement.shape), speed.reshape(velocity.shape)


def solution(mesh):
    in_specs = (
        P(None, None, "mesh", "sub"),
        P(None, None, "mesh", "sub"),
        P(None, "mesh", "sub"),
        P(None, "mesh", "sub"),
        P(),
        P(None, "mesh", "sub"),
        P("mesh", "sub", None, None),
        P("mesh", "sub", None),
        P(None, "mesh", "sub", None, None),
        P(None, "mesh", "sub"),
    )
    out_specs = (P(None, None, "mesh", "sub"), P(None, None, "mesh", "sub"))
    return jax.shard_map(shards, mesh=mesh, in_specs=in_specs, out_specs=out_specs, check_vma=False)
```

```python
import functools

import jax
import jax.numpy as jnp
from jax import lax
from jax.experimental import pallas as pl
from jax.experimental.pallas import tpu as pltpu
from jax.sharding import PartitionSpec as P

TIME_STEP = 0.1
MESH = pl.DeviceIdType.MESH
ROWS = 8
LANES = 128
DIRECTIONS = ((0, 1), (0, -1), (1, 0), (-1, 0), (1, 1), (1, -1), (-1, 1), (-1, -1))
SLOT = {d: i for i, d in enumerate(DIRECTIONS)}
PAD = 24


def kernel(
    n_mesh,
    n_sub,
    steps,
    stiff_hbm,
    owners_hbm,
    disp_hbm,
    vel_hbm,
    mass_hbm,
    moduli_hbm,
    surf_hbm,
    facets_hbm,
    penalty_hbm,
    pairs_hbm,
    out_disp,
    out_vel,
    stiff,
    owners,
    own,
    vel,
    mass,
    surf,
    pairs,
    table,
    packed,
    arrived,
    wide,
    found,
    local_sem,
    table_send,
    table_recv,
    halo_send,
    halo_recv,
):
    q, s = lax.axis_index("mesh"), lax.axis_index("sub")

    def at(dq, ds):
        return (lax.rem(q + dq + n_mesh, n_mesh), lax.rem(s + ds + n_sub, n_sub))

    chunks = table.shape[1] // 8
    copies = [
        pltpu.make_async_copy(src, dst, local_sem.at[i])
        for i, (src, dst) in enumerate(
            (
                (disp_hbm, own.at[pl.ds(0, 48)]),
                (moduli_hbm, own.at[pl.ds(48, 16)]),
                (facets_hbm, table.at[q, pl.ds(0, 6 * chunks)]),
                (penalty_hbm, table.at[q, pl.ds(6 * chunks, chunks)]),
                (pairs_hbm, pairs),
                (surf_hbm, surf),
                (vel_hbm, vel),
                (mass_hbm, mass),
                (stiff_hbm, stiff),
                (owners_hbm, owners),
            )
        )
    ]
    barrier = pltpu.get_barrier_semaphore()
    partners = [at(*d) for d in DIRECTIONS if d[1] != 0] + [at(d, 0) for d in range(1, n_mesh)]
    for device in partners:
        pl.semaphore_signal(barrier, inc=1, device_id=device, device_id_type=MESH)
    for copy in copies:
        copy.start()

    lane = lax.broadcasted_iota(jnp.int32, (ROWS, LANES), 1)

    def pack(step, planes, count):
        left = jnp.zeros((ROWS, LANES), jnp.float32)
        right = left
        for p in range(count):
            plane = planes[p]
            left = jnp.where(lane == p, pltpu.roll(plane, p, 1) if p else plane, left)
            right = jnp.where(lane == p, pltpu.roll(plane, p + 1, 1), right)
        packed[step, 0] = left
        packed[step, 1] = right
        packed[step, 2] = own[pl.ds(0, 8, stride=8), :]
        packed[step, 3] = own[pl.ds(7, 8, stride=8), :]

    def halo(step):
        made = []
        for i, (dq, ds) in enumerate(DIRECTIONS):
            source = (2 if dq < 0 else 3) if dq else (0 if ds < 0 else 1)
            made.append(
                pltpu.make_async_remote_copy(
                    src_ref=packed.at[step, source],
                    dst_ref=arrived.at[step, i],
                    send_sem=halo_send.at[step, i],
                    recv_sem=halo_recv.at[step, i],
                    device_id=at(dq, ds),
                    device_id_type=MESH,
                )
            )
        return made

    for o in range(n_mesh):
        table[o, pl.ds(7 * chunks, chunks), :] = jnp.zeros((chunks, LANES), jnp.float32)
    copies[0].wait()
    copies[1].wait()
    pack(0, [own[pl.ds(8 * p, 8), :] for p in range(8)], 8)
    copies[2].wait()
    copies[3].wait()
    pl.semaphore_wait(barrier, len(partners))
    halos = halo(0)
    for copy in halos:
        copy.start()
    shared = []
    for d in range(1, n_mesh):
        used = table.at[q, pl.ds(0, 7 * chunks)]
        shared.append(
            pltpu.make_async_remote_copy(
                src_ref=used,
                dst_ref=used,
                send_sem=table_send.at[d - 1],
                recv_sem=table_recv.at[d - 1],
                device_id=at(d, 0),
                device_id_type=MESH,
            )
        )
    for copy in shared:
        copy.start()
    for copy in copies[4:]:
        copy.wait()
    inverse = [TIME_STEP / mass[pl.ds(8 * a, 8), :] for a in range(2)]

    def gather(step):
        for b in range(ROWS):
            owner = owners[step, b]
            index = jnp.broadcast_to(pairs[pl.ds(step * ROWS + b, 1), :], (ROWS, LANES))
            chunk, place = index >> 7, index & 127
            total = jnp.zeros((ROWS, LANES), jnp.float32)
            for k in range(chunks):
                rows = table[owner, pl.ds(k, 8, stride=chunks), :]
                picked = jnp.take_along_axis(rows, place, axis=1, mode="promise_in_bounds")
                total = jnp.where(chunk == k, picked, total)
            found[step, pl.ds(8 * b, 8), :] = total

    def spread(step, planes, count):
        from_left, from_right = arrived[step, SLOT[(0, 1)]], arrived[step, SLOT[(0, -1)]]
        for p in range(count):
            plane = planes[p]
            before = pltpu.roll(from_left, LANES - p, 1) if p else from_left
            after = pltpu.roll(from_right, LANES - 1 - p, 1)
            rows = pl.ds(p * PAD + 8, 8)
            wide[0, rows, :] = jnp.where(lane == 0, before, pltpu.roll(plane, 1, 1))
            wide[1, rows, :] = plane
            wide[2, rows, :] = jnp.where(lane == LANES - 1, after, pltpu.roll(plane, LANES - 1, 1))
        for dq, row in ((1, 7), (-1, 16)):
            centre = arrived[step, SLOT[(dq, 0)]]
            west, east = arrived[step, SLOT[(dq, 1)]], arrived[step, SLOT[(dq, -1)]]
            rows = pl.ds(row, 8, stride=PAD)
            wide[0, rows, :] = pltpu.roll(jnp.where(lane == LANES - 1, west, centre), 1, 1)
            wide[1, rows, :] = centre
            wide[2, rows, :] = pltpu.roll(jnp.where(lane == 0, east, centre), LANES - 1, 1)

    def shifted(p, di, dj):
        return wide[dj + 1, pl.ds(p * PAD + 8 + di, 8), :]

    scales = {}
    planes = [own[pl.ds(8 * p, 8), :] for p in range(8)]
    for step in range(steps):
        if step == 0:
            for copy in shared:
                copy.wait_recv()
        gather(step)
        for copy in halos:
            copy.wait_recv()
        spread(step, planes, 8 if step == 0 else 6)
        if step == 0:
            both = {
                (di, dj): shifted(6, di, dj) + shifted(7, di, dj) for di in (-1, 0, 1) for dj in (-1, 0, 1)
            }
            for b in (0, 1):
                for e in (0, 1):
                    scales[b, e] = 0.125 * (
                        (both[-b, -e] + both[-b, 1 - e]) + (both[1 - b, -e] + both[1 - b, 1 - e])
                    )
        force = [None] * 6
        for b in (0, 1):
            for e in (0, 1):
                sums = [None] * 6
                for corner in range(8):
                    a2, b2, e2 = corner >> 2, (corner >> 1) & 1, corner & 1
                    for m2 in range(3):
                        value = shifted(2 * m2 + a2, b2 - b, e2 - e)
                        for a in (0, 1):
                            for m in range(3):
                                row = 3 * (4 * a + 2 * b + e) + m
                                term = stiff[row, 3 * corner + m2] * value
                                o = 2 * m + a
                                sums[o] = term if sums[o] is None else sums[o] + term
                for o in range(6):
                    term = scales[b, e] * sums[o]
                    force[o] = term if force[o] is None else force[o] + term
        facet = [found[step, pl.ds(c, 8, stride=8), :] for c in range(7)]
        points = [surf[pl.ds(8 * m, 8), :] + planes[2 * m] for m in range(3)]
        gap = sum(facet[3 + m] * (points[m] - facet[m]) for m in range(3))
        strength = facet[6] * jnp.maximum(-gap, 0.0)
        last = step == steps - 1
        fresh = []
        for o in range(6):
            m, a = o // 2, o % 2
            net = facet[3 + m] * strength - force[o] if a == 0 else -force[o]
            rows = pl.ds(8 * o, 8)
            speed = vel[rows, :] + inverse[a] * net
            moved = planes[o] + TIME_STEP * speed
            fresh.append(moved)
            if last:
                out_vel[rows, :] = speed
                out_disp[rows, :] = moved
            else:
                vel[rows, :] = speed
                own[rows, :] = moved
        for copy in halos:
            copy.wait_send()
        planes = fresh
        if not last:
            pack(step + 1, planes, 6)
            halos = halo(step + 1)
            for copy in halos:
                copy.start()
    for copy in shared:
        copy.wait_send()


def shards(
    displacement,
    velocity,
    node_mass,
    moduli,
    stiffness,
    surface_ref,
    facets,
    penalty,
    owners,
    facet_pairs,
):
    steps = owners.shape[0]
    width = facets.shape[3]
    n_mesh, n_sub = lax.axis_size("mesh"), lax.axis_size("sub")
    assert displacement.shape == (3, 2, ROWS, LANES)
    f32 = jnp.float32
    out = pltpu.VMEM((6 * ROWS, LANES), f32)
    anywhere = pl.BlockSpec(memory_space=pl.ANY)
    vmem = pl.BlockSpec(memory_space=pltpu.VMEM)
    dma = pltpu.SemaphoreType.DMA
    moved, speed = pl.pallas_call(
        functools.partial(kernel, n_mesh, n_sub, steps),
        out_shape=(out, out),
        in_specs=[anywhere] * 10,
        out_specs=(vmem, vmem),
        scratch_shapes=[
            pltpu.SMEM((24, 24), f32),
            pltpu.SMEM((steps, ROWS), jnp.int32),
            pltpu.VMEM((8 * ROWS, LANES), f32),
            pltpu.VMEM((6 * ROWS, LANES), f32),
            pltpu.VMEM((2 * ROWS, LANES), f32),
            pltpu.VMEM((3 * ROWS, LANES), f32),
            pltpu.VMEM((steps * ROWS, LANES), jnp.int32),
            pltpu.VMEM((n_mesh, 8 * width // LANES, LANES), f32),
            pltpu.VMEM((steps, 4, ROWS, LANES), f32),
            pltpu.VMEM((steps, 8, ROWS, LANES), f32),
            pltpu.VMEM((3, 8 * PAD, LANES), f32),
            pltpu.VMEM((steps, 8 * ROWS, LANES), f32),
            dma((10,)),
            dma((n_mesh - 1,)),
            dma((n_mesh - 1,)),
            dma((steps, 8)),
            dma((steps, 8)),
        ],
        compiler_params=pltpu.CompilerParams(collective_id=0, has_side_effects=True),
    )(
        stiffness,
        owners.reshape(steps, ROWS),
        displacement.reshape(6 * ROWS, LANES),
        velocity.reshape(6 * ROWS, LANES),
        node_mass.reshape(2 * ROWS, LANES),
        moduli.reshape(2 * ROWS, LANES),
        surface_ref.reshape(3 * ROWS, LANES),
        facets.transpose(0, 2, 1, 3).reshape(6 * width // LANES, LANES),
        penalty.reshape(width // LANES, LANES),
        facet_pairs.reshape(steps * ROWS, LANES),
    )
    return moved.reshape(displacement.shape), speed.reshape(velocity.shape)


def solution(mesh):
    in_specs = (
        P(None, None, "mesh", "sub"),
        P(None, None, "mesh", "sub"),
        P(None, "mesh", "sub"),
        P(None, "mesh", "sub"),
        P(),
        P(None, "mesh", "sub"),
        P("mesh", "sub", None, None),
        P("mesh", "sub", None),
        P(None, "mesh", "sub", None, None),
        P(None, "mesh", "sub"),
    )
    out_specs = (P(None, None, "mesh", "sub"), P(None, None, "mesh", "sub"))
    return jax.shard_map(shards, mesh=mesh, in_specs=in_specs, out_specs=out_specs, check_vma=False)
```

```python
import functools

import jax
import jax.numpy as jnp
from jax import lax
from jax.experimental import pallas as pl
from jax.experimental.pallas import tpu as pltpu
from jax.sharding import PartitionSpec as P

TIME_STEP = 0.1
MESH = pl.DeviceIdType.MESH
ROWS = 8
LANES = 128
DIRECTIONS = ((1, 1), (1, -1), (-1, 1), (-1, -1), (1, 0), (-1, 0), (0, 1), (0, -1))
SLOT = {d: i for i, d in enumerate(DIRECTIONS)}
PAD = 24


def kernel(
    n_mesh,
    n_sub,
    steps,
    stiff_hbm,
    owners_hbm,
    disp_hbm,
    vel_hbm,
    mass_hbm,
    moduli_hbm,
    surf_hbm,
    facets_hbm,
    penalty_hbm,
    pairs_hbm,
    out_disp,
    out_vel,
    stiff,
    owners,
    own,
    vel,
    mass,
    surf,
    pairs,
    table,
    packed,
    arrived,
    wide,
    found,
    local_sem,
    table_send,
    table_recv,
    halo_send,
    halo_recv,
):
    q, s = lax.axis_index("mesh"), lax.axis_index("sub")

    def at(dq, ds):
        return (lax.rem(q + dq + n_mesh, n_mesh), lax.rem(s + ds + n_sub, n_sub))

    chunks = table.shape[1] // 8
    copies = [
        pltpu.make_async_copy(src, dst, local_sem.at[i])
        for i, (src, dst) in enumerate(
            (
                (disp_hbm, own.at[pl.ds(0, 48)]),
                (moduli_hbm, own.at[pl.ds(48, 16)]),
                (facets_hbm, table.at[q, pl.ds(0, 6 * chunks)]),
                (penalty_hbm, table.at[q, pl.ds(6 * chunks, chunks)]),
                (pairs_hbm, pairs),
                (surf_hbm, surf),
                (vel_hbm, vel),
                (mass_hbm, mass),
                (stiff_hbm, stiff),
                (owners_hbm, owners),
            )
        )
    ]
    barrier = pltpu.get_barrier_semaphore()
    partners = [at(*d) for d in DIRECTIONS if d[1] != 0] + [at(d, 0) for d in range(1, n_mesh)]
    for device in partners:
        pl.semaphore_signal(barrier, inc=1, device_id=device, device_id_type=MESH)
    for copy in copies:
        copy.start()

    lane = lax.broadcasted_iota(jnp.int32, (ROWS, LANES), 1)

    def pack(step, planes, count):
        left = jnp.zeros((ROWS, LANES), jnp.float32)
        right = left
        for p in range(count):
            plane = planes[p]
            left = jnp.where(lane == p, pltpu.roll(plane, p, 1) if p else plane, left)
            right = jnp.where(lane == p, pltpu.roll(plane, p + 1, 1), right)
        packed[step, 0] = left
        packed[step, 1] = right

    def pack_rows(step):
        packed[step, 2] = own[pl.ds(0, 8, stride=8), :]
        packed[step, 3] = own[pl.ds(7, 8, stride=8), :]

    def halo(step):
        made = []
        for i, (dq, ds) in enumerate(DIRECTIONS):
            source = (2 if dq < 0 else 3) if dq else (0 if ds < 0 else 1)
            made.append(
                pltpu.make_async_remote_copy(
                    src_ref=packed.at[step, source],
                    dst_ref=arrived.at[step, i],
                    send_sem=halo_send.at[step, i],
                    recv_sem=halo_recv.at[step, i],
                    device_id=at(dq, ds),
                    device_id_type=MESH,
                )
            )
        return made

    for o in range(n_mesh):
        table[o, pl.ds(7 * chunks, chunks), :] = jnp.zeros((chunks, LANES), jnp.float32)
    copies[0].wait()
    copies[1].wait()
    pack_rows(0)
    pack(0, [own[pl.ds(8 * p, 8), :] for p in range(8)], 8)
    copies[2].wait()
    copies[3].wait()
    pl.semaphore_wait(barrier, len(partners))
    halos = halo(0)
    for copy in halos:
        copy.start()
    shared = []
    for d in range(1, n_mesh):
        used = table.at[q, pl.ds(0, 7 * chunks)]
        shared.append(
            pltpu.make_async_remote_copy(
                src_ref=used,
                dst_ref=used,
                send_sem=table_send.at[d - 1],
                recv_sem=table_recv.at[d - 1],
                device_id=at(d, 0),
                device_id_type=MESH,
            )
        )
    for copy in shared:
        copy.start()
    for copy in copies[4:]:
        copy.wait()
    inverse = [TIME_STEP / mass[pl.ds(8 * a, 8), :] for a in range(2)]

    def gather(step):
        for b in range(ROWS):
            owner = owners[step, b]
            index = jnp.broadcast_to(pairs[pl.ds(step * ROWS + b, 1), :], (ROWS, LANES))
            chunk, place = index >> 7, index & 127
            total = jnp.zeros((ROWS, LANES), jnp.float32)
            for k in range(chunks):
                rows = table[owner, pl.ds(k, 8, stride=chunks), :]
                picked = jnp.take_along_axis(rows, place, axis=1, mode="promise_in_bounds")
                total = jnp.where(chunk == k, picked, total)
            found[step, pl.ds(8 * b, 8), :] = total

    def spread_middle(step, planes, count):
        for p in range(count):
            wide[1, pl.ds(p * PAD + 8, 8), :] = planes[p]
        for dq, row in ((1, 7), (-1, 16)):
            wide[1, pl.ds(row, 8, stride=PAD), :] = arrived[step, SLOT[(dq, 0)]]

    def spread_sides(step, turned, count):
        from_left, from_right = arrived[step, SLOT[(0, 1)]], arrived[step, SLOT[(0, -1)]]
        for p in range(count):
            before = pltpu.roll(from_left, LANES - p, 1) if p else from_left
            after = pltpu.roll(from_right, LANES - 1 - p, 1)
            rows = pl.ds(p * PAD + 8, 8)
            wide[0, rows, :] = jnp.where(lane == 0, before, turned[p][0])
            wide[2, rows, :] = jnp.where(lane == LANES - 1, after, turned[p][1])
        for dq, row in ((1, 7), (-1, 16)):
            centre = arrived[step, SLOT[(dq, 0)]]
            west, east = arrived[step, SLOT[(dq, 1)]], arrived[step, SLOT[(dq, -1)]]
            rows = pl.ds(row, 8, stride=PAD)
            wide[0, rows, :] = pltpu.roll(jnp.where(lane == LANES - 1, west, centre), 1, 1)
            wide[2, rows, :] = pltpu.roll(jnp.where(lane == 0, east, centre), LANES - 1, 1)

    def shifted(p, di, dj):
        return wide[dj + 1, pl.ds(p * PAD + 8 + di, 8), :]

    scales = {}
    planes = [own[pl.ds(8 * p, 8), :] for p in range(8)]
    for step in range(steps):
        if step == 0:
            for copy in shared:
                copy.wait_recv()
        gather(step)
        facet = [found[step, pl.ds(c, 8, stride=8), :] for c in range(7)]
        points = [surf[pl.ds(8 * m, 8), :] + planes[2 * m] for m in range(3)]
        gap = sum(facet[3 + m] * (points[m] - facet[m]) for m in range(3))
        strength = facet[6] * jnp.maximum(-gap, 0.0)
        push = [facet[3 + m] * strength for m in range(3)]
        count = 8 if step == 0 else 6
        turned = [(pltpu.roll(p, 1, 1), pltpu.roll(p, LANES - 1, 1)) for p in planes[:count]]
        sums = {(b, e): [None] * 6 for b in (0, 1) for e in (0, 1)}

        def accumulate(middle):
            for b, e in sums:
                for corner in range(8):
                    a2, b2, e2 = corner >> 2, (corner >> 1) & 1, corner & 1
                    if (e2 == e) != middle:
                        continue
                    for m2 in range(3):
                        value = shifted(2 * m2 + a2, b2 - b, e2 - e)
                        for o in range(6):
                            row = 3 * (4 * (o % 2) + 2 * b + e) + o // 2
                            term = stiff[row, 3 * corner + m2] * value
                            before = sums[b, e][o]
                            sums[b, e][o] = term if before is None else before + term

        for d in ((1, 0), (-1, 0)):
            halos[SLOT[d]].wait_recv()
        spread_middle(step, planes, count)
        accumulate(True)
        for d in DIRECTIONS:
            if d[1] != 0:
                halos[SLOT[d]].wait_recv()
        spread_sides(step, turned, count)
        if step == 0:
            both = {
                (di, dj): shifted(6, di, dj) + shifted(7, di, dj) for di in (-1, 0, 1) for dj in (-1, 0, 1)
            }
            for b in (0, 1):
                for e in (0, 1):
                    scales[b, e] = 0.125 * (
                        (both[-b, -e] + both[-b, 1 - e]) + (both[1 - b, -e] + both[1 - b, 1 - e])
                    )
        accumulate(False)
        force = [None] * 6
        for b, e in sums:
            for o in range(6):
                term = scales[b, e] * sums[b, e][o]
                force[o] = term if force[o] is None else force[o] + term
        last = step == steps - 1
        fresh = []
        for o in range(6):
            m, a = o // 2, o % 2
            net = push[m] - force[o] if a == 0 else -force[o]
            rows = pl.ds(8 * o, 8)
            speed = vel[rows, :] + inverse[a] * net
            moved = planes[o] + TIME_STEP * speed
            fresh.append(moved)
            if last:
                out_vel[rows, :] = speed
                out_disp[rows, :] = moved
            else:
                vel[rows, :] = speed
                own[rows, :] = moved
        planes = fresh
        sent = halos
        if not last:
            halos = halo(step + 1)
            pack_rows(step + 1)
            for d in DIRECTIONS:
                if d[0] != 0:
                    halos[SLOT[d]].start()
            pack(step + 1, planes, 6)
            for d in DIRECTIONS:
                if d[0] == 0:
                    halos[SLOT[d]].start()
        for copy in sent:
            copy.wait_send()
    for copy in shared:
        copy.wait_send()


def flush(moved, speed, out_moved, out_speed, sem):
    copies = [
        pltpu.make_async_copy(src, dst, sem.at[i])
        for i, (src, dst) in enumerate(((moved, out_moved), (speed, out_speed)))
    ]
    for copy in copies:
        copy.start()
    for copy in copies:
        copy.wait()


def shards(
    displacement,
    velocity,
    node_mass,
    moduli,
    stiffness,
    surface_ref,
    facets,
    penalty,
    owners,
    facet_pairs,
):
    steps = owners.shape[0]
    width = facets.shape[3]
    n_mesh, n_sub = lax.axis_size("mesh"), lax.axis_size("sub")
    assert displacement.shape == (3, 2, ROWS, LANES)
    f32 = jnp.float32
    out = pltpu.VMEM((6 * ROWS, LANES), f32)
    anywhere = pl.BlockSpec(memory_space=pl.ANY)
    vmem = pl.BlockSpec(memory_space=pltpu.VMEM)
    dma = pltpu.SemaphoreType.DMA
    moved, speed = pl.pallas_call(
        functools.partial(kernel, n_mesh, n_sub, steps),
        out_shape=(out, out),
        in_specs=[anywhere] * 10,
        out_specs=(vmem, vmem),
        scratch_shapes=[
            pltpu.SMEM((24, 24), f32),
            pltpu.SMEM((steps, ROWS), jnp.int32),
            pltpu.VMEM((8 * ROWS, LANES), f32),
            pltpu.VMEM((6 * ROWS, LANES), f32),
            pltpu.VMEM((2 * ROWS, LANES), f32),
            pltpu.VMEM((3 * ROWS, LANES), f32),
            pltpu.VMEM((steps * ROWS, LANES), jnp.int32),
            pltpu.VMEM((n_mesh, 8 * width // LANES, LANES), f32),
            pltpu.VMEM((steps, 4, ROWS, LANES), f32),
            pltpu.VMEM((steps, 8, ROWS, LANES), f32),
            pltpu.VMEM((3, 8 * PAD, LANES), f32),
            pltpu.VMEM((steps, 8 * ROWS, LANES), f32),
            dma((10,)),
            dma((n_mesh - 1,)),
            dma((n_mesh - 1,)),
            dma((steps, 8)),
            dma((steps, 8)),
        ],
        compiler_params=pltpu.CompilerParams(collective_id=0, has_side_effects=True),
    )(
        stiffness,
        owners.reshape(steps, ROWS),
        displacement.reshape(6 * ROWS, LANES),
        velocity.reshape(6 * ROWS, LANES),
        node_mass.reshape(2 * ROWS, LANES),
        moduli.reshape(2 * ROWS, LANES),
        surface_ref.reshape(3 * ROWS, LANES),
        facets.transpose(0, 2, 1, 3).reshape(6 * width // LANES, LANES),
        penalty.reshape(width // LANES, LANES),
        facet_pairs.reshape(steps * ROWS, LANES),
    )
    moved, speed = pl.pallas_call(
        flush,
        out_shape=[jax.ShapeDtypeStruct((6 * ROWS, LANES), f32)] * 2,
        in_specs=[anywhere, anywhere],
        out_specs=[anywhere, anywhere],
        scratch_shapes=[dma((2,))],
        compiler_params=pltpu.CompilerParams(vmem_limit_bytes=1 << 20),
    )(pltpu.with_memory_space_constraint(moved, pltpu.VMEM), pltpu.with_memory_space_constraint(speed, pltpu.VMEM))
    return moved.reshape(displacement.shape), speed.reshape(velocity.shape)


def solution(mesh):
    in_specs = (
        P(None, None, "mesh", "sub"),
        P(None, None, "mesh", "sub"),
        P(None, "mesh", "sub"),
        P(None, "mesh", "sub"),
        P(),
        P(None, "mesh", "sub"),
        P("mesh", "sub", None, None),
        P("mesh", "sub", None),
        P(None, "mesh", "sub", None, None),
        P(None, "mesh", "sub"),
    )
    out_specs = (P(None, None, "mesh", "sub"), P(None, None, "mesh", "sub"))
    return jax.shard_map(shards, mesh=mesh, in_specs=in_specs, out_specs=out_specs, check_vma=False)
```

```python
import functools

import jax
import jax.numpy as jnp
from jax import lax
from jax.experimental import pallas as pl
from jax.experimental.pallas import tpu as pltpu
from jax.sharding import PartitionSpec as P

TIME_STEP = 0.1
MESH = pl.DeviceIdType.MESH
ROWS = 8
LANES = 128
DIRECTIONS = ((1, 1), (1, -1), (-1, 1), (-1, -1), (1, 0), (-1, 0), (0, 1), (0, -1))
SLOT = {d: i for i, d in enumerate(DIRECTIONS)}
PAD = 24


def kernel(
    n_mesh,
    n_sub,
    steps,
    stiff_hbm,
    owners_hbm,
    disp_hbm,
    vel_hbm,
    mass_hbm,
    moduli_hbm,
    surf_hbm,
    facets_hbm,
    penalty_hbm,
    pairs_hbm,
    out_disp,
    out_vel,
    stiff,
    owners,
    own,
    vel,
    mass,
    surf,
    pairs,
    table,
    packed,
    arrived,
    wide,
    found,
    local_sem,
    table_send,
    table_recv,
    halo_send,
    halo_recv,
):
    q, s = lax.axis_index("mesh"), lax.axis_index("sub")

    def at(dq, ds):
        return (lax.rem(q + dq + n_mesh, n_mesh), lax.rem(s + ds + n_sub, n_sub))

    chunks = table.shape[1] // 8
    copies = [
        pltpu.make_async_copy(src, dst, local_sem.at[i])
        for i, (src, dst) in enumerate(
            (
                (disp_hbm, own.at[pl.ds(0, 48)]),
                (moduli_hbm, own.at[pl.ds(48, 16)]),
                (facets_hbm, table.at[q, pl.ds(0, 6 * chunks)]),
                (penalty_hbm, table.at[q, pl.ds(6 * chunks, chunks)]),
                (pairs_hbm, pairs),
                (surf_hbm, surf),
                (vel_hbm, vel),
                (mass_hbm, mass),
                (stiff_hbm, stiff),
                (owners_hbm, owners),
            )
        )
    ]
    barrier = pltpu.get_barrier_semaphore()
    partners = [at(*d) for d in DIRECTIONS if d[1] != 0] + [at(d, 0) for d in range(1, n_mesh)]
    for device in partners:
        pl.semaphore_signal(barrier, inc=1, device_id=device, device_id_type=MESH)
    for copy in copies:
        copy.start()

    lane = lax.broadcasted_iota(jnp.int32, (ROWS, LANES), 1)

    def pack(step, planes, count):
        left = jnp.zeros((ROWS, LANES), jnp.float32)
        right = left
        for p in range(count):
            plane = planes[p]
            left = jnp.where(lane == p, pltpu.roll(plane, p, 1) if p else plane, left)
            right = jnp.where(lane == p, pltpu.roll(plane, p + 1, 1), right)
        packed[step, 0] = left
        packed[step, 1] = right

    def pack_rows(step):
        packed[step, 2] = own[pl.ds(0, 8, stride=8), :]
        packed[step, 3] = own[pl.ds(7, 8, stride=8), :]

    def halo(step):
        made = []
        for i, (dq, ds) in enumerate(DIRECTIONS):
            source = (2 if dq < 0 else 3) if dq else (0 if ds < 0 else 1)
            made.append(
                pltpu.make_async_remote_copy(
                    src_ref=packed.at[step, source],
                    dst_ref=arrived.at[step, i],
                    send_sem=halo_send.at[step, i],
                    recv_sem=halo_recv.at[step, i],
                    device_id=at(dq, ds),
                    device_id_type=MESH,
                )
            )
        return made

    for o in range(n_mesh):
        table[o, pl.ds(7 * chunks, chunks), :] = jnp.zeros((chunks, LANES), jnp.float32)
    copies[0].wait()
    copies[1].wait()
    pack_rows(0)
    pack(0, [own[pl.ds(8 * p, 8), :] for p in range(8)], 8)
    pl.semaphore_wait(barrier, len(partners))
    halos = halo(0)
    for copy in halos:
        copy.start()
    copies[2].wait()
    copies[3].wait()
    shared = []
    for d in range(1, n_mesh):
        used = table.at[q, pl.ds(0, 7 * chunks)]
        shared.append(
            pltpu.make_async_remote_copy(
                src_ref=used,
                dst_ref=used,
                send_sem=table_send.at[d - 1],
                recv_sem=table_recv.at[d - 1],
                device_id=at(d, 0),
                device_id_type=MESH,
            )
        )
    for copy in shared:
        copy.start()
    for copy in copies[4:]:
        copy.wait()
    inverse = [TIME_STEP / mass[pl.ds(8 * a, 8), :] for a in range(2)]

    def gather(step):
        for b in range(ROWS):
            owner = owners[step, b]
            index = jnp.broadcast_to(pairs[pl.ds(step * ROWS + b, 1), :], (ROWS, LANES))
            chunk, place = index >> 7, index & 127
            total = jnp.zeros((ROWS, LANES), jnp.float32)
            for k in range(chunks):
                rows = table[owner, pl.ds(k, 8, stride=chunks), :]
                picked = jnp.take_along_axis(rows, place, axis=1, mode="promise_in_bounds")
                total = jnp.where(chunk == k, picked, total)
            found[step, pl.ds(8 * b, 8), :] = total

    def spread_middle(step, planes, count):
        for p in range(count):
            wide[1, pl.ds(p * PAD + 8, 8), :] = planes[p]
        for dq, row in ((1, 7), (-1, 16)):
            wide[1, pl.ds(row, 8, stride=PAD), :] = arrived[step, SLOT[(dq, 0)]]

    def spread_sides(step, turned, count):
        from_left, from_right = arrived[step, SLOT[(0, 1)]], arrived[step, SLOT[(0, -1)]]
        for p in range(count):
            before = pltpu.roll(from_left, LANES - p, 1) if p else from_left
            after = pltpu.roll(from_right, LANES - 1 - p, 1)
            rows = pl.ds(p * PAD + 8, 8)
            wide[0, rows, :] = jnp.where(lane == 0, before, turned[p][0])
            wide[2, rows, :] = jnp.where(lane == LANES - 1, after, turned[p][1])
        for dq, row in ((1, 7), (-1, 16)):
            centre = arrived[step, SLOT[(dq, 0)]]
            west, east = arrived[step, SLOT[(dq, 1)]], arrived[step, SLOT[(dq, -1)]]
            rows = pl.ds(row, 8, stride=PAD)
            wide[0, rows, :] = pltpu.roll(jnp.where(lane == LANES - 1, west, centre), 1, 1)
            wide[2, rows, :] = pltpu.roll(jnp.where(lane == 0, east, centre), LANES - 1, 1)

    def shifted(p, di, dj):
        return wide[dj + 1, pl.ds(p * PAD + 8 + di, 8), :]

    scales = {}
    planes = [own[pl.ds(8 * p, 8), :] for p in range(8)]
    for step in range(steps):
        if step == 0:
            for copy in shared:
                copy.wait_recv()
        gather(step)
        facet = [found[step, pl.ds(c, 8, stride=8), :] for c in range(7)]
        points = [surf[pl.ds(8 * m, 8), :] + planes[2 * m] for m in range(3)]
        gap = sum(facet[3 + m] * (points[m] - facet[m]) for m in range(3))
        strength = facet[6] * jnp.maximum(-gap, 0.0)
        push = [facet[3 + m] * strength for m in range(3)]
        count = 8 if step == 0 else 6
        turned = [(pltpu.roll(p, 1, 1), pltpu.roll(p, LANES - 1, 1)) for p in planes[:count]]
        sums = {(b, e): [None] * 6 for b in (0, 1) for e in (0, 1)}

        def accumulate(middle):
            for b, e in sums:
                for corner in range(8):
                    a2, b2, e2 = corner >> 2, (corner >> 1) & 1, corner & 1
                    if (e2 == e) != middle:
                        continue
                    for m2 in range(3):
                        value = shifted(2 * m2 + a2, b2 - b, e2 - e)
                        for o in range(6):
                            row = 3 * (4 * (o % 2) + 2 * b + e) + o // 2
                            term = stiff[row, 3 * corner + m2] * value
                            before = sums[b, e][o]
                            sums[b, e][o] = term if before is None else before + term

        for d in ((1, 0), (-1, 0)):
            halos[SLOT[d]].wait_recv()
        spread_middle(step, planes, count)
        accumulate(True)
        for d in DIRECTIONS:
            if d[1] != 0:
                halos[SLOT[d]].wait_recv()
        spread_sides(step, turned, count)
        if step == 0:
            both = {
                (di, dj): shifted(6, di, dj) + shifted(7, di, dj) for di in (-1, 0, 1) for dj in (-1, 0, 1)
            }
            for b in (0, 1):
                for e in (0, 1):
                    scales[b, e] = 0.125 * (
                        (both[-b, -e] + both[-b, 1 - e]) + (both[1 - b, -e] + both[1 - b, 1 - e])
                    )
        accumulate(False)
        force = [None] * 6
        for b, e in sums:
            for o in range(6):
                term = scales[b, e] * sums[b, e][o]
                force[o] = term if force[o] is None else force[o] + term
        last = step == steps - 1
        fresh = []
        for o in range(6):
            m, a = o // 2, o % 2
            net = push[m] - force[o] if a == 0 else -force[o]
            rows = pl.ds(8 * o, 8)
            speed = vel[rows, :] + inverse[a] * net
            moved = planes[o] + TIME_STEP * speed
            fresh.append(moved)
            if last:
                out_vel[rows, :] = speed
                out_disp[rows, :] = moved
            else:
                vel[rows, :] = speed
                own[rows, :] = moved
        planes = fresh
        sent = halos
        if not last:
            halos = halo(step + 1)
            pack_rows(step + 1)
            for d in DIRECTIONS:
                if d[0] != 0:
                    halos[SLOT[d]].start()
            pack(step + 1, planes, 6)
            for d in DIRECTIONS:
                if d[0] == 0:
                    halos[SLOT[d]].start()
        for copy in sent:
            copy.wait_send()
    for copy in shared:
        copy.wait_send()


def flush(moved, speed, out_moved, out_speed, sem):
    copies = [
        pltpu.make_async_copy(src, dst, sem.at[i])
        for i, (src, dst) in enumerate(((moved, out_moved), (speed, out_speed)))
    ]
    for copy in copies:
        copy.start()
    for copy in copies:
        copy.wait()


def shards(
    displacement,
    velocity,
    node_mass,
    moduli,
    stiffness,
    surface_ref,
    facets,
    penalty,
    owners,
    facet_pairs,
):
    steps = owners.shape[0]
    width = facets.shape[3]
    n_mesh, n_sub = lax.axis_size("mesh"), lax.axis_size("sub")
    assert displacement.shape == (3, 2, ROWS, LANES)
    f32 = jnp.float32
    out = pltpu.VMEM((6 * ROWS, LANES), f32)
    anywhere = pl.BlockSpec(memory_space=pl.ANY)
    vmem = pl.BlockSpec(memory_space=pltpu.VMEM)
    dma = pltpu.SemaphoreType.DMA
    moved, speed = pl.pallas_call(
        functools.partial(kernel, n_mesh, n_sub, steps),
        out_shape=(out, out),
        in_specs=[anywhere] * 10,
        out_specs=(vmem, vmem),
        scratch_shapes=[
            pltpu.SMEM((24, 24), f32),
            pltpu.SMEM((steps, ROWS), jnp.int32),
            pltpu.VMEM((8 * ROWS, LANES), f32),
            pltpu.VMEM((6 * ROWS, LANES), f32),
            pltpu.VMEM((2 * ROWS, LANES), f32),
            pltpu.VMEM((3 * ROWS, LANES), f32),
            pltpu.VMEM((steps * ROWS, LANES), jnp.int32),
            pltpu.VMEM((n_mesh, 8 * width // LANES, LANES), f32),
            pltpu.VMEM((steps, 4, ROWS, LANES), f32),
            pltpu.VMEM((steps, 8, ROWS, LANES), f32),
            pltpu.VMEM((3, 8 * PAD, LANES), f32),
            pltpu.VMEM((steps, 8 * ROWS, LANES), f32),
            dma((10,)),
            dma((n_mesh - 1,)),
            dma((n_mesh - 1,)),
            dma((steps, 8)),
            dma((steps, 8)),
        ],
        compiler_params=pltpu.CompilerParams(collective_id=0, has_side_effects=True),
    )(
        stiffness,
        owners.reshape(steps, ROWS),
        displacement.reshape(6 * ROWS, LANES),
        velocity.reshape(6 * ROWS, LANES),
        node_mass.reshape(2 * ROWS, LANES),
        moduli.reshape(2 * ROWS, LANES),
        surface_ref.reshape(3 * ROWS, LANES),
        facets.transpose(0, 2, 1, 3).reshape(6 * width // LANES, LANES),
        penalty.reshape(width // LANES, LANES),
        facet_pairs.reshape(steps * ROWS, LANES),
    )
    moved, speed = pl.pallas_call(
        flush,
        out_shape=[jax.ShapeDtypeStruct((6 * ROWS, LANES), f32)] * 2,
        in_specs=[anywhere, anywhere],
        out_specs=[anywhere, anywhere],
        scratch_shapes=[dma((2,))],
        compiler_params=pltpu.CompilerParams(vmem_limit_bytes=1 << 20),
    )(pltpu.with_memory_space_constraint(moved, pltpu.VMEM), pltpu.with_memory_space_constraint(speed, pltpu.VMEM))
    return moved.reshape(displacement.shape), speed.reshape(velocity.shape)


def solution(mesh):
    in_specs = (
        P(None, None, "mesh", "sub"),
        P(None, None, "mesh", "sub"),
        P(None, "mesh", "sub"),
        P(None, "mesh", "sub"),
        P(),
        P(None, "mesh", "sub"),
        P("mesh", "sub", None, None),
        P("mesh", "sub", None),
        P(None, "mesh", "sub", None, None),
        P(None, "mesh", "sub"),
    )
    out_specs = (P(None, None, "mesh", "sub"), P(None, None, "mesh", "sub"))
    return jax.shard_map(shards, mesh=mesh, in_specs=in_specs, out_specs=out_specs, check_vma=False)
```
